32 devices in a mesh: lat: 4 (over y, x), lon: 8 (over z, core).
Axes of the slice: x: 2, y: 2, z: 4, core: 2. Of those that a mesh axis runs over, the one named last changes fastest.
Arguments:
- right_side: float32 [512, 1024], P('lat', 'lon'), may hold values from -8 to 8
- surface_term: float32 [512, 1024], P('lat', 'lon'), may hold values from 0.0002 to 0.002
- east_coupling: float32 [512, 1024], P('lat', 'lon'), may hold values from 0.3 to 3
- north_coupling: float32 [512, 1024], P('lat', 'lon'), may hold values from 0.3 to 3
- neast_coupling: float32 [512, 1024], P('lat', 'lon'), may hold values from 0.1 to 0.5
- nwest_coupling: float32 [512, 1024], P('lat', 'lon'), may hold values from 0.1 to 0.5
- land_sea: int32 [512, 1024], P('lat', 'lon'), may hold values from 0 to 1, as said below
- fold_map: int32 [1024], P('lon'), may hold values from 0 to 1023, as said below
Outputs:
- solution: float32 [512, 1024], P('lat', 'lon')
- residual: float32 [512, 1024], P('lat', 'lon')
The draws below stay inside these ranges and needn't reach their ends.
Inputs may be any that keep to these rules, and one draw needn't show every extreme that they name: fold_map[j] = (c - j) mod 1024 for one odd c: an involution of the columns with no fixed point. land_sea is 0 or 1; land lies in bands of 8 columns, each over one range of rows.
All inputs are finite; a program needn't handle non-finite values.
Results may differ from the reference program's by a relative error of at most 0.0015.
Values sent between devices are 32-bit elements.
A program may use at most 64 MiB of HBM per device.

```python
import math
import jax
import jax.numpy as jnp
from jax import lax

ITERS = 8
NLAT = 512
NLON = 1024


def draw_right_side(key, part):
    noise_key, scale_key = jax.random.split(jax.random.fold_in(key, 11))
    row_block = jnp.arange(NLAT) // 150
    col_block = jnp.arange(NLON) // 64
    block_scales = jnp.exp(jax.random.uniform(scale_key, (NLAT // 150 + 1, NLON // 64 + 1), jnp.float32, math.log(0.1), math.log(3.0)))
    cell_scale = block_scales[row_block[:, None], col_block[None, :]]
    noise_values = jax.random.normal(noise_key, (NLAT, NLON), jnp.float32)
    return jnp.clip(noise_values * cell_scale, -8.0, 8.0)


def draw_land_sea(key, part):
    first_key, second_key, third_key = jax.random.split(jax.random.fold_in(key, 37), 3)
    band_count = NLON // 8
    continent = (jax.random.randint(first_key, (band_count,), 0, 3, jnp.int32) == 0) | (jnp.arange(band_count) == 0)
    start_row = jax.random.randint(second_key, (band_count,), 0, NLAT // 2, jnp.int32)
    extent = jax.random.randint(third_key, (band_count,), NLAT // 8 + 1, NLAT // 2 + 1, jnp.int32)
    band_of = jnp.arange(NLON, dtype=jnp.int32) // 8
    rows = jnp.arange(NLAT, dtype=jnp.int32)[:, None]
    land = continent[band_of][None, :] & (rows >= start_row[band_of][None, :]) & (rows < (start_row + extent)[band_of][None, :])
    return jnp.where(land, 0, 1).astype(jnp.int32)


def draw_fold_map(key, part):
    offset = 2 * jax.random.randint(jax.random.fold_in(key, 23), (), 0, NLON // 2, jnp.int32) + 1
    return (offset - jnp.arange(NLON, dtype=jnp.int32)) % NLON


def levels(rng, shape, cuts, low, top_value):
    factor_of = 1.0
    for dim, parts in cuts:
        draws = jax.random.uniform(jax.random.fold_in(jax.random.fold_in(rng, 6), dim), (parts,), jnp.float32, low / len(cuts), top_value / len(cuts))
        factor_of = factor_of * jnp.repeat(jnp.exp(draws), shape[dim] // parts).reshape((-1,) + (1,) * (len(shape) - 1 - dim))
    return factor_of


def setup_inputs(seed: int = 0) -> dict:
    keys = jax.random.split(jax.random.key(seed), 9)
    return {
        "right_side": draw_right_side(jax.random.fold_in(keys[8], 71), 0),
        "surface_term": jnp.clip(jnp.exp(math.log(0.002) - 2.3025852 * jax.random.uniform(keys[1], (NLAT, NLON), jnp.float32) ** levels(keys[1], (NLAT, NLON), ((0, 4), (1, 8)), -0.2, 0.2)), 0.0002, 0.002),
        "east_coupling": jnp.clip(jnp.exp(math.log(3.0) - 2.3025851 * jax.random.uniform(keys[2], (NLAT, NLON), jnp.float32) ** levels(keys[2], (NLAT, NLON), ((0, 4), (1, 8)), -0.2, 0.2)), 0.3, 3.0),
        "north_coupling": jnp.clip(jnp.exp(math.log(3.0) - 2.3025851 * jax.random.uniform(keys[3], (NLAT, NLON), jnp.float32) ** levels(keys[3], (NLAT, NLON), ((0, 4), (1, 8)), -0.2, 0.2)), 0.3, 3.0),
        "neast_coupling": jnp.clip(jnp.exp(math.log(0.5) - 1.609438 * jax.random.uniform(keys[4], (NLAT, NLON), jnp.float32) ** levels(keys[4], (NLAT, NLON), ((0, 4), (1, 8)), -0.2, 0.2)), 0.1, 0.5),
        "nwest_coupling": jnp.clip(jnp.exp(math.log(0.5) - 1.609438 * jax.random.uniform(keys[5], (NLAT, NLON), jnp.float32) ** levels(keys[5], (NLAT, NLON), ((0, 4), (1, 8)), -0.2, 0.2)), 0.1, 0.5),
        "land_sea": draw_land_sea(jax.random.fold_in(keys[8], 71), 0),
        "fold_map": draw_fold_map(jax.random.fold_in(keys[8], 71), 0),
    }


OFFSETS = ((0, 1), (0, -1), (1, 0), (-1, 0), (1, 1), (-1, -1), (1, -1), (-1, 1))
COUPLINGS = ((1, 0, 0), (1, 0, -1), (2, 0, 0), (2, -1, 0), (3, 0, 0), (3, -1, -1), (4, 0, 0), (4, -1, 1))

def interior(padded, row_step, col_step):
    row_count = padded.shape[-2] - 2
    col_count = padded.shape[-1] - 2
    return padded[..., 1 + row_step:1 + row_step + row_count, 1 + col_step:1 + col_step + col_count]

def stencil_weights(padded):
    ocean_pad = padded[0]
    centre = interior(ocean_pad, 0, 0)
    weight_list = []
    open_sum = jnp.zeros_like(centre)
    for (layer_index, row_step, col_step), (row_off, col_off) in zip(COUPLINGS, OFFSETS):
        edge_value = interior(padded[layer_index], row_step, col_step)
        weight_list.append(edge_value * centre * interior(ocean_pad, row_off, col_off))
        open_sum = open_sum + edge_value
    return (jnp.stack(weight_list), open_sum)

def neighbour_sum(weights, padded_field):
    accumulated = jnp.zeros_like(weights[0])
    for position, (row_off, col_off) in enumerate(OFFSETS):
        accumulated = accumulated + weights[position] * interior(padded_field, row_off, col_off)
    return accumulated

def pad_grid(values):
    wrapped = jnp.concatenate([values[..., -1:], values, values[..., :1]], axis=-1)
    zero_row = jnp.zeros_like(wrapped[..., :1, :])
    return jnp.concatenate([zero_row, wrapped, zero_row], axis=-2)

def line_solve(lower_band, middle_band, upper_band, values):
    solved = lax.linalg.tridiagonal_solve(lower_band.T, middle_band.T, upper_band.T, values.T[:, :, None])
    return solved[:, :, 0].T

def reference(right_side, surface_term, east_coupling, north_coupling, neast_coupling, nwest_coupling, land_sea, fold_map):
    ocean = land_sea.astype(jnp.float32)
    row_ids = lax.broadcasted_iota(jnp.int32, ocean.shape, 0)
    top_row = jnp.where(row_ids == ocean.shape[0] - 1, 1.0, 0.0).astype(jnp.float32)
    open_rows = 1.0 - top_row
    stacked = jnp.stack([ocean, east_coupling, north_coupling * open_rows, neast_coupling * open_rows, nwest_coupling * open_rows])
    weights, open_sum = stencil_weights(pad_grid(stacked))
    top_north = north_coupling[-1]
    fold_open = 0.5 * (top_north + jnp.take(top_north, fold_map))
    fold_weight = fold_open * ocean[-1] * jnp.take(ocean[-1], fold_map)
    diagonal = ocean * (surface_term + open_sum + top_row * fold_open[None]) + (1.0 - ocean)
    line_diagonal = ocean * (surface_term + weights[2] + weights[3]) + (1.0 - ocean)
    lower_band = -weights[3]
    upper_band = -weights[2]

    def operate(field):
        fold_term = fold_weight * jnp.take(field[-1], fold_map)
        return diagonal * field - neighbour_sum(weights, pad_grid(field)) - top_row * fold_term[None]
    residual = ocean * right_side
    solution = jnp.zeros_like(residual)
    precond = line_solve(lower_band, line_diagonal, upper_band, residual)
    direction = precond
    product_now = jnp.sum(residual * precond)
    for iteration in range(ITERS):
        image_field = operate(direction)
        step_length = product_now / jnp.sum(direction * image_field)
        solution = solution + step_length * direction
        residual = residual - step_length * image_field
        if iteration + 1 < ITERS:
            precond = line_solve(lower_band, line_diagonal, upper_band, residual)
            product_next = jnp.sum(residual * precond)
            direction = precond + product_next / product_now * direction
            product_now = product_next
    return (solution, residual)
```

```python
import functools

import jax
import jax.numpy as jnp
from jax import lax
from jax.experimental import pallas as pl
from jax.experimental.pallas import tpu as pltpu
from jax.sharding import PartitionSpec as P

ITERS = 8
SUB = 8
FIELDS = 6
MESH = pl.DeviceIdType.MESH


def iota(shape, dim):
    return lax.broadcasted_iota(jnp.int32, shape, dim)


def east(x):
    return pltpu.roll(x, x.shape[-1] - 1, x.ndim - 1)


def west(x):
    return pltpu.roll(x, 1, x.ndim - 1)


def from_above(x):
    return pltpu.roll(x, SUB - 1, 0)


def from_below(x):
    return pltpu.roll(x, 1, 0)


def alternate(size):
    ring = []
    for i in range(1, size // 2 + 1):
        ring += [size - i, i]
    return list(dict.fromkeys([*ring, 0]))


def kernel(
    lat_count,
    lon_count,
    right_ref,
    surface_ref,
    east_ref,
    north_ref,
    neast_ref,
    nwest_ref,
    land_ref,
    map_ref,
    sol_out,
    res_out,
    w_e,
    w_w,
    w_n,
    w_s,
    w_ne,
    w_sw,
    w_nw,
    w_se,
    diag,
    f_a,
    f_g,
    resp0,
    resp1,
    top_resp,
    c_mid,
    c_east,
    c_west,
    y_ref,
    w_ref,
    res_ref,
    r_mid,
    y_mid,
    z_mid,
    sol_ref,
    s_mid,
    z_pair,
    k_pair,
    fields,
    given,
    land_buf,
    map_buf,
    big_msg,
    small_msg,
    big_recv,
    small_recv,
    stat_msg,
    stat_recv,
    whole,
    msg,
    recv,
    back_msg,
    back_recv,
    in_sem,
    big_send,
    big_arrive,
    small_send,
    small_arrive,
    stat_send,
    stat_arrive,
    send_sem,
    recv_sem,
    back_send,
    back_arrive,
):
    pairs = lon_count // 2
    n_own = lat_count * pairs
    lat = lax.axis_index("lat")
    lon = lax.axis_index("lon")
    pair = lon // 2
    core = lax.rem(lon, 2)
    me = lat * pairs + pair
    depth, _, width = sol_ref.shape
    rows = depth * SUB // lat_count
    subs = SUB // lat_count
    halo = ITERS
    own = 2 * width // lat_count
    big = own + halo
    rest = width - big
    left = big - rest
    band = big_msg.shape[1]
    thin = small_msg.shape[1]
    seg = band // subs
    half = depth // 2
    top = depth - 1
    odd = lax.rem(lat, 2)
    is_owner = core == 1

    lats = [lax.rem(lat + d, lat_count) for d in range(lat_count)]
    owners = [2 * lax.rem(pair + d, pairs) + 1 for d in range(pairs)]
    few = n_own <= 64
    peers = [(p, q) for q in alternate(pairs) for p in alternate(lat_count) if p or q]

    def to_owners(act):
        if few:
            for p, q in peers:
                act((lats[p], owners[q]))
            return

        def one(step, carry):
            peer = lax.rem(me + step, n_own)
            act((peer // pairs, 2 * lax.rem(peer, pairs) + 1))
            return carry

        lax.fori_loop(1, n_own, one, 0)

    left_place = (2 * core, 2 * pair + 1)
    right_place = (2 * core + 1, 2 * pair + 1)
    next_place = (lax.rem(2 * core + 2, lat_count), 2 * lax.rem(pair + core, pairs) + 1)
    back_pair = lax.rem(pair + core + pairs - 1, pairs)
    prev_place = (lax.rem(2 * core + 3, lat_count), 2 * back_pair + 1)

    barrier = pltpu.get_barrier_semaphore()

    def greet(place):
        pl.semaphore_signal(barrier, inc=1, device_id=place, device_id_type=MESH)

    @pl.when(is_owner)
    def _():
        to_owners(greet)
        last_lat = jnp.where(lat == lat_count - 1, 1, 0)
        plain = 2 * lax.rem(pair + last_lat, pairs)
        for a in range(lat_count):
            greet((a, plain))

    @pl.when(core == 0)
    def _():
        for place in (left_place, right_place, next_place, prev_place):
            greet(place)

    sources = (right_ref, surface_ref, east_ref, north_ref, neast_ref, nwest_ref)
    loads = [
        pltpu.make_async_copy(ref, given.at[i], in_sem.at[i]) for i, ref in enumerate(sources)
    ]
    loads.append(pltpu.make_async_copy(land_ref, land_buf, in_sem.at[FIELDS]))
    map_load = pltpu.make_async_copy(map_ref, map_buf, in_sem.at[FIELDS + 1])
    for copy in loads:
        copy.start()
    map_load.start()
    for copy in loads:
        copy.wait()
    map_load.wait()

    wide = iota((SUB, width), 1)
    zero = jnp.zeros((SUB, width), jnp.float32)
    for v in range(rows // SUB):
        sl = slice(v * SUB, (v + 1) * SUB)
        given[1, sl] = given[1, sl] * land_buf[sl].astype(jnp.float32)
    for s in range(subs):
        for v in range(depth // SUB):
            sl = slice(s * depth + v * SUB, s * depth + (v + 1) * SUB)
            for c in range(FIELDS // 2):
                first, second = given[2 * c, sl], given[2 * c + 1, sl]
                at = s * seg + c * depth + v * SUB
                to = slice(at, at + SUB)
                big_msg[0, to] = jnp.where(wide < big, first, pltpu.roll(second, rest, 1))
                big_msg[1, to] = jnp.where(wide >= rest, first, pltpu.roll(second, big, 1))
        for v in range(half // SUB):
            acc_l, acc_r, acc_n, acc_p = zero, zero, zero, zero
            for i in range(FIELDS):
                for e in range(2):
                    rows_at = pl.ds(s * depth + 2 * v * SUB + e, SUB, stride=2)
                    piece = given[i, rows_at, :]
                    slot = i + FIELDS * e
                    hit = wide // halo == slot
                    lane = halo * slot
                    acc_n = jnp.where(hit, pltpu.roll(piece, (lane + halo) % width, 1), acc_n)
                    moved = pltpu.roll(piece, lane, 1) if lane else piece
                    acc_p = jnp.where(hit, moved, acc_p)
                    if i % 2 == 1:
                        slot = i // 2 + FIELDS // 2 * e
                        hit = wide // left == slot
                        lane = left * slot
                        moved = pltpu.roll(piece, lane, 1) if lane else piece
                        acc_l = jnp.where(hit, moved, acc_l)
                        moved = pltpu.roll(piece, (lane + left) % width, 1)
                        acc_r = jnp.where(hit, moved, acc_r)
            at = s * seg + FIELDS // 2 * depth + v * SUB
            big_msg[0, at : at + SUB] = acc_l
            big_msg[1, at : at + SUB] = acc_r
            at = s * half + v * SUB
            small_msg[0, at : at + SUB] = acc_n
            small_msg[1, at : at + SUB] = acc_p

    here_big = pl.ds(pl.multiple_of(lat * band, SUB), band)
    here_thin = pl.ds(pl.multiple_of(lat * thin, SUB), thin)

    def big_copy(side, place):
        return pltpu.make_async_remote_copy(
            src_ref=big_msg.at[side],
            dst_ref=big_recv.at[here_big],
            send_sem=big_send.at[side],
            recv_sem=big_arrive.at[lat],
            device_id=place,
            device_id_type=MESH,
        )

    def thin_copy(side, place):
        return pltpu.make_async_remote_copy(
            src_ref=small_msg.at[side],
            dst_ref=small_recv.at[here_thin],
            send_sem=small_send.at[side],
            recv_sem=small_arrive.at[lat],
            device_id=place,
            device_id_type=MESH,
        )

    @pl.when(is_owner)
    def _():
        pl.semaphore_wait(barrier, n_own - 1 + lat_count)

    @pl.when(core == 0)
    def _():
        pl.semaphore_wait(barrier, lat_count)

    outgoing = [
        (big_copy(0, left_place), jnp.logical_and(is_owner, lat == 2)),
        (big_copy(1, right_place), jnp.logical_and(is_owner, lat == 3)),
        (thin_copy(0, next_place), None),
        (thin_copy(1, prev_place), jnp.logical_and(is_owner, lat == 1)),
    ]
    for copy, stays in outgoing:
        if stays is None:
            copy.start()
        else:
            pl.when(jnp.logical_not(stays))(copy.start)

    @pl.when(outgoing[0][1])
    def _():
        big_recv[here_big] = big_msg[0]

    @pl.when(outgoing[1][1])
    def _():
        big_recv[here_big] = big_msg[1]

    @pl.when(outgoing[3][1])
    def _():
        small_recv[here_thin] = small_msg[1]

    def back_copy(a):
        return pltpu.make_async_remote_copy(
            src_ref=back_msg.at[a * rows : (a + 1) * rows],
            dst_ref=back_recv.at[odd],
            send_sem=back_send.at[a],
            recv_sem=back_arrive.at[odd],
            device_id=(a, 2 * pair + lat // 2),
            device_id_type=MESH,
        )

    def solve_columns():
        for a in range(lat_count):

            @pl.when(jnp.logical_or(lat != a, lat < 2))
            def _(a=a):
                pltpu.make_async_remote_copy(
                    src_ref=big_msg.at[0],
                    dst_ref=big_recv.at[a * band : (a + 1) * band],
                    send_sem=big_send.at[0],
                    recv_sem=big_arrive.at[a],
                    device_id=left_place,
                    device_id_type=MESH,
                ).wait_recv()

            @pl.when(jnp.logical_or(lat != a, lat != 1))
            def _(a=a):
                pltpu.make_async_remote_copy(
                    src_ref=small_msg.at[0],
                    dst_ref=small_recv.at[a * thin : (a + 1) * thin],
                    send_sem=small_send.at[0],
                    recv_sem=small_arrive.at[a],
                    device_id=next_place,
                    device_id_type=MESH,
                ).wait_recv()

        def between(low, size):
            return (wide >= low) & (wide < low + size)

        native = between(odd * rest, big)
        side_low = (1 - odd) * (width - halo)
        inside = native | between(side_low, halo)
        main = between(left + odd * (rest - left), rest)
        edge_low = odd * (width - left)
        edge = between(edge_low, left)

        def turned(x, shift):
            return pltpu.roll(x, lax.rem(shift + 2 * width, width), 1)

        for k in range(depth):
            e = k % 2
            strip = small_recv[pl.ds(k // 2, SUB, stride=half), :]
            spill = big_recv[pl.ds(FIELDS // 2 * depth + k // 2, SUB, stride=seg), :]
            for c in range(FIELDS // 2):
                packed = big_recv[pl.ds(c * depth + k, SUB, stride=seg), :]
                out = []
                for i in (2 * c, 2 * c + 1):
                    strip_at = turned(strip, side_low - halo * (i + FIELDS * e))
                    out.append(jnp.where(inside, strip_at, 0.0))
                fields[2 * c, k] = jnp.where(native, packed, out[0])
                spill_at = turned(spill, edge_low - left * (c + FIELDS // 2 * e))
                value = jnp.where(edge, spill_at, out[1])
                fields[2 * c + 1, k] = jnp.where(main, turned(packed, big - odd * left), value)

        def field(index, k):
            if index == FIELDS:
                return jnp.where(fields[1, k] > 0.0, 1.0, 0.0)
            return fields[index, k]

        is_top = iota((SUB, width), 0) == SUB - 1

        def closed(index, k):
            value = field(index, k)
            return jnp.where(is_top, 0.0, value) if k == top else value

        def above(index, k):
            return field(index, k + 1) if k < top else from_above(field(index, 0))

        n_prev, ne_prev, nw_prev = (from_below(closed(i, top)) for i in (3, 4, 5))
        for k in range(depth):
            ocean = field(FIELDS, k)
            ocean_north = above(FIELDS, k)
            e_now, n_now, ne_now, nw_now = field(2, k), closed(3, k), closed(4, k), closed(5, k)
            we = e_now * ocean * east(ocean)
            wn = n_now * ocean * ocean_north
            wne = ne_now * ocean * east(ocean_north)
            wnw = nw_now * ocean * west(ocean_north)
            w_e[k] = we
            w_w[k] = west(we)
            w_n[k] = wn
            w_ne[k] = wne
            w_nw[k] = wnw
            sw, se = west(wne), east(wnw)
            if k < top:
                w_s[k + 1] = wn
                w_sw[k + 1] = sw
                w_se[k + 1] = se
            else:
                w_s[0] = from_below(wn)
                w_sw[0] = from_below(sw)
                w_se[0] = from_below(se)
            open_sum = (
                e_now
                + west(e_now)
                + n_now
                + n_prev
                + ne_now
                + west(ne_prev)
                + nw_now
                + east(nw_prev)
            )
            diag[k] = field(1, k) + ocean * open_sum + (1.0 - ocean)
            n_prev, ne_prev, nw_prev = n_now, ne_now, nw_now
            res_ref[k] = ocean * field(0, k)
            for ref in (r_mid, y_mid, z_mid, sol_ref, s_mid):
                ref[k] = zero
            z_pair[1, k] = zero
            k_pair[1, k] = zero

        def surface(k):
            return field(1, k) + (1.0 - field(FIELDS, k))

        low = surface(0) + w_s[0]
        high = surface(top) + w_n[top]
        for k in range(half):
            up, j = k, top - k
            g_low = 1.0 / (low + w_n[up])
            g_high = 1.0 / (high + w_s[j])
            f_g[up] = g_low
            f_g[j] = g_high
            if k < half - 1:
                f_a[up + 1] = w_n[up] * g_low
                f_a[j - 1] = w_s[j] * g_high
                low = surface(up + 1) + w_n[up] * (low * g_low)
                high = surface(j - 1) + w_s[j] * (high * g_high)
        mid = w_n[half - 1]
        inv_det = 1.0 / (low * high + mid * (low + high))
        mid_ll = (high + mid) * inv_det
        mid_lh = mid * inv_det
        mid_hh = (low + mid) * inv_det

        def line(read, out, u_ref):
            y, z = read(0), read(top)
            u_ref[0] = y
            u_ref[top] = z
            for k in range(1, half):
                j = top - k
                y = read(k) + f_a[k] * y
                z = read(j) + f_a[j] * z
                u_ref[k] = y
                u_ref[j] = z
            x = mid_ll * y + mid_lh * z
            v = mid_lh * y + mid_hh * z
            out[half - 1] = x
            out[half] = v
            for k in range(half - 2, -1, -1):
                j = top - k
                x = f_g[k] * u_ref[k] + f_a[k + 1] * x
                v = f_g[j] * u_ref[j] + f_a[j - 1] * v
                out[k] = x
                out[j] = v

        line(lambda k: w_s[0] if k == 0 else zero, resp0, y_ref)
        line(lambda k: w_n[top] if k == top else zero, resp1, y_ref)

        a, b, c, d = resp0[0], resp1[0], resp0[top], resp1[top]
        plan = []
        stride = 1
        while stride < SUB:
            cb, db = pltpu.roll(c, stride, 0), pltpu.roll(d, stride, 0)
            aa, ba = pltpu.roll(a, SUB - stride, 0), pltpu.roll(b, SUB - stride, 0)
            m00, m01 = 1.0 - a * db, -b * aa
            m10, m11 = -c * db, 1.0 - d * aa
            inv = 1.0 / (m00 * m11 - m01 * m10)
            i00, i01, i10, i11 = m11 * inv, -m01 * inv, -m10 * inv, m00 * inv
            t0, t1 = i00 * a + i01 * c, i00 * b + i01 * d
            t2, t3 = i10 * a + i11 * c, i10 * b + i11 * d
            plan.append((stride, i00, i01, i10, i11, t0, t1, t2, t3))
            a, b, c, d = t0 * cb, t1 * ba, t2 * cb, t3 * ba
            stride *= 2

        def interface(p, q):
            for stride, i00, i01, i10, i11, t0, t1, t2, t3 in plan:
                qb = pltpu.roll(q, stride, 0)
                pa = pltpu.roll(p, SUB - stride, 0)
                p, q = (
                    (i00 * p + i01 * q) + (t0 * qb + t1 * pa),
                    (i10 * p + i11 * q) + (t2 * qb + t3 * pa),
                )
            return from_below(q), from_above(p)

        def solve(read, u_ref):
            line(read, u_ref, u_ref)
            below, over = interface(u_ref[0], u_ref[top])

            def finish(k):
                value = u_ref[k] + below * resp0[k] + over * resp1[k]
                u_ref[k] = value
                return value

            return finish

        def walk(finish):
            last = finish(top)
            first = finish(0)
            last = (last, east(last), west(last))
            first = (first, east(first), west(first))
            prev = tuple(from_below(x) for x in last)
            now = first
            for k in range(depth):
                if k < top - 1:
                    value = finish(k + 1)
                    nxt = (value, east(value), west(value))
                elif k == top - 1:
                    nxt = last
                else:
                    nxt = tuple(from_above(x) for x in first)
                yield k, prev, now, nxt
                prev, now = now, nxt

        def column_sum(x):
            return jnp.sum(x, axis=0, keepdims=True)

        lane = iota((1, width), 1)
        relative = lax.rem(lane - odd * own + width, width)
        own_row = relative < own

        unit = jnp.where(is_top, 1.0, 0.0)
        h_mid, h_east = zero, zero
        for k, prev, now, nxt in walk(solve(lambda k: unit if k == top else zero, top_resp)):
            middle = diag[k] * now[0] - w_n[k] * nxt[0] - w_s[k] * prev[0]
            eastern = -(w_e[k] * now[1] + w_ne[k] * nxt[1] + w_se[k] * prev[1])
            c_mid[k] = middle
            c_east[k] = eastern
            c_west[k] = -(w_w[k] * now[2] + w_nw[k] * nxt[2] + w_sw[k] * prev[2])
            h_mid = h_mid + now[0] * middle
            h_east = h_east + now[0] * eastern

        def both(native_row, other_row):
            return jnp.where(own_row, native_row, pltpu.roll(other_row, own, 1))

        def last_row(x):
            return x[SUB - 1 :]

        stat_msg[0] = both(last_row(top_resp[top]), column_sum(h_mid))
        stat_msg[1] = both(column_sum(h_east), last_row(field(3, top)))
        stat_msg[2] = both(last_row(field(FIELDS, top)), jnp.zeros((1, width), jnp.float32))
        stat_recv[me] = stat_msg[...]

        def stat_start(place):
            pltpu.make_async_remote_copy(
                src_ref=stat_msg,
                dst_ref=stat_recv.at[me],
                send_sem=stat_send,
                recv_sem=stat_arrive,
                device_id=place,
                device_id_type=MESH,
            ).start()

        to_owners(stat_start)

        def send_rows(parity):
            def start(place):
                pltpu.make_async_remote_copy(
                    src_ref=msg.at[parity],
                    dst_ref=recv.at[parity, me],
                    send_sem=send_sem.at[parity],
                    recv_sem=recv_sem.at[parity],
                    device_id=place,
                    device_id_type=MESH,
                ).start()

            to_owners(start)

        def wait_for(every, sent, arrived):
            pltpu.make_async_remote_copy(
                src_ref=every,
                dst_ref=every,
                send_sem=sent,
                recv_sem=arrived,
                device_id=next_place,
                device_id_type=MESH,
            ).wait()

        lanes = iota((lon_count, width), 1)
        rows_id = iota((lon_count, width), 0)

        def assemble(read):
            lefts, rights = [], []
            for block in range(lon_count):
                spot = 2 * (block % 2) * pairs + block // 2
                lefts.append(read(spot))
                rights.append(read(spot + pairs))
            lefts = jnp.concatenate(lefts, axis=0)
            rights = jnp.concatenate(rights, axis=0)
            native_rows = jnp.where(lanes < own, lefts, rights)
            other_rows = pltpu.roll(jnp.where(lanes < own, rights, lefts), own, 1)
            return native_rows, other_rows

        total_cols = lon_count * width
        turn = lax.rem(map_buf[0] + lon * width, total_cols)
        back = total_cols - 1 - turn
        row_shift = back // width
        lane_shift = lax.rem(back, width)
        turn_index = width - 1 - lax.rem(lanes + lane_shift, width)

        def facing(x):
            flipped = jnp.concatenate(
                [x[b : b + 1] for b in range(lon_count - 1, -1, -1)], axis=0
            )
            moved = jnp.take_along_axis(flipped, turn_index, axis=1)
            first = pltpu.roll(moved, lax.rem(lon_count - row_shift, lon_count), 0)
            second = pltpu.roll(moved, lon_count - 1 - row_shift, 0)
            return jnp.where(lanes + lane_shift < width, first, second)

        block_row = 2 * pair + lat // 2
        odd_home = jnp.where(lanes < own // 2, 1, 0)
        even_home = jnp.where(lanes >= width - own // 2, -1, 0)
        home = block_row + odd * odd_home + (1 - odd) * even_home
        pick = rows_id == lax.rem(home + lon_count, lon_count)

        def window(x):
            return jnp.sum(jnp.where(pick, x, 0.0), axis=0, keepdims=True)

        def spread(x):
            return jnp.broadcast_to(x, (SUB, width))

        def total(x):
            return jnp.sum(x, keepdims=True)

        def advance(side, length, ratio, length2, ratio2, turned_row):
            g1, q1 = spread(ratio * length), spread(1.0 - ratio)
            g2, q2 = spread(ratio2 * length2), spread(1.0 - ratio2)
            rho, rho2 = spread(ratio), spread(ratio2)
            phi = spread(turned_row)
            for k in range(depth):
                z = z_pair[side, k]
                image = k_pair[side, k] - top_resp[k] * phi
                old, older = sol_ref[k], s_mid[k]
                toward = rho * z - g1 * image + q1 * z_mid[k]
                between_sol = rho * old + g1 * z + q1 * older
                z_mid[k] = toward
                s_mid[k] = between_sol
                sol_ref[k] = rho2 * between_sol + g2 * toward + q2 * old

        def block_step(step, carry):
            length_old, ratio_old, mu_old, nu_old, length_mid, ratio_mid, phi_old = carry
            parity = lax.rem(step, 2)
            z_ref, k_ref = z_pair.at[parity], k_pair.at[parity]
            acc = [zero] * 9

            def stencil(k, prev, now, nxt):
                return (
                    (diag[k] * now[0] - w_e[k] * now[1] - w_w[k] * now[2])
                    - (w_n[k] * nxt[0] + w_ne[k] * nxt[1] + w_nw[k] * nxt[2])
                    - (w_s[k] * prev[0] + w_se[k] * prev[1] + w_sw[k] * prev[2])
                )

            for k, prev, now, nxt in walk(solve(lambda k: res_ref[k], z_ref)):
                value = stencil(k, prev, now, nxt)
                y_ref[k] = value
                acc[k % 2] = acc[k % 2] + res_ref[k] * now[0]
                acc[2 + k % 2] = acc[2 + k % 2] + now[0] * value
            for k, prev, now, nxt in walk(solve(lambda k: y_ref[k], k_ref)):
                value = stencil(k, prev, now, nxt)
                w_ref[k] = value
                acc[4 + k % 2] = acc[4 + k % 2] + y_ref[k] * now[0]
                acc[6 + k % 2] = acc[6 + k % 2] + now[0] * value
                acc[8] = acc[8] + top_resp[k] * value
            parts = [
                total(jnp.where(own_row, acc[2 * i] + acc[2 * i + 1], 0.0)) for i in range(4)
            ]
            sums = jnp.zeros((1, width), jnp.float32)
            for i in range(4):
                sums = jnp.where(relative == own + i, parts[i], sums)
            msg[parity, 0] = both(last_row(z_ref[top]), last_row(k_ref[top]))
            msg[parity, 1] = jnp.where(own_row, column_sum(acc[8]), sums)
            recv[parity, me] = msg[parity]
            send_rows(parity)
            advance(1 - parity, length_mid, ratio_mid, length_old, ratio_old, phi_old)

            @pl.when(step == 0)
            def _():
                wait_for(stat_recv.at[0 : n_own - 1], stat_send, stat_arrive)
                h0, h1 = assemble(lambda spot: stat_recv[spot, 0])
                h2, north = assemble(lambda spot: stat_recv[spot, 1])
                ocean, _unused = assemble(lambda spot: stat_recv[spot, 2])
                fold_open = 0.5 * (north + facing(north))
                fold_own = fold_open * ocean
                fold_far = fold_own * facing(ocean)
                for i, x in enumerate(
                    (h0, h1, 2.0 * h2, fold_own, fold_far, facing(h0), facing(fold_own))
                ):
                    whole[i] = x

            wait_for(recv.at[parity, 0 : n_own - 1], send_sem.at[parity], recv_sem.at[parity])
            tau0, tau1 = assemble(lambda spot: recv[parity, spot, 0])
            tail, rest_rows = assemble(lambda spot: recv[parity, spot, 1])
            h0, h1, h2, fold_own, fold_far, h0_facing, own_facing = (whole[i] for i in range(7))
            tau0_facing, tau1_facing = facing(tau0), facing(tau1)
            phi0 = fold_far * tau0_facing - fold_own * tau0
            phi0_facing = fold_far * tau0 - own_facing * tau0_facing
            top1 = tau1 - h0 * phi0
            phi1 = fold_far * (tau1_facing - h0_facing * phi0_facing) - fold_own * top1
            shifted = east(phi0)
            shifted = jnp.where(
                lanes == width - 1, pltpu.roll(shifted, lon_count - 1, 0), shifted
            )
            rest_lane = lax.rem(lanes, own)

            def moment(i, x):
                return total(jnp.where(rest_lane == i, rest_rows, 0.0) + x)

            m0 = moment(0, 0.0)
            m1 = moment(1, -tau0 * phi0)
            m2 = moment(2, phi0 * (h0 * phi0 - 2.0 * tau1))
            m3 = moment(3, phi0 * (h1 * phi0 + h2 * shifted - 2.0 * tail) - top1 * phi1)
            phi0_row, phi1_row = window(phi0), window(phi1)

            start = step == 0
            length = m0 / m1
            factor = ratio_old * length_old
            ratio = jnp.where(start, 1.0, 1.0 / (1.0 - (length * m0) / (factor * mu_old)))
            cross = jnp.where(start, 0.0, -m0 / factor)
            cross2 = jnp.where(start, 0.0, (ratio_old * cross - m1) / factor)
            q = 1.0 - ratio
            gain = ratio * length
            mu = (
                gain * gain * m2
                - ratio * ratio * m0
                + q * q * mu_old
                - 2.0 * gain * q * cross
            )
            nu = (
                ratio * ratio * m1
                + gain * gain * m3
                + q * q * nu_old
                - 2.0 * ratio * gain * m2
                + 2.0 * ratio * q * cross
                - 2.0 * gain * q * cross2
            )
            length2 = mu / nu
            ratio2 = 1.0 / (1.0 - (length2 * mu) / (gain * m0))
            rho, g1, q1 = spread(ratio), spread(gain), spread(q)
            rho2, g2, q2 = spread(ratio2), spread(ratio2 * length2), spread(1.0 - ratio2)
            p_mid, p_east, p_west = (
                spread(phi0_row),
                spread(east(phi0_row)),
                spread(west(phi0_row)),
            )
            phi1_top = jnp.where(is_top, spread(phi1_row), 0.0)
            phi0_top = jnp.where(is_top, p_mid, 0.0)
            for k in range(depth):
                image = y_ref[k]
                second = w_ref[k] - (c_mid[k] * p_mid + c_east[k] * p_east + c_west[k] * p_west)
                if k == top:
                    image = image - phi0_top
                    second = second - phi1_top
                res = res_ref[k]
                between_res = rho * res - g1 * image + q1 * r_mid[k]
                toward = rho * image - g1 * second + q1 * y_mid[k]
                r_mid[k] = between_res
                y_mid[k] = toward
                res_ref[k] = rho2 * between_res - g2 * toward + q2 * res
            return (length2, ratio2, mu, nu, length, ratio, phi0_row)

        one = jnp.ones((1, 1), jnp.float32)
        nil = jnp.zeros((1, 1), jnp.float32)
        carry = (nil, one, one, one, nil, one, jnp.zeros((1, width), jnp.float32))
        carry = lax.fori_loop(0, ITERS // 2, block_step, carry)
        length2, ratio2, _, _, length, ratio, phi_row = carry
        advance((ITERS // 2 - 1) % 2, length, ratio, length2, ratio2, phi_row)

        for k in range(depth):
            value = jnp.where(own_row, sol_ref[k], pltpu.roll(res_ref[k], own, 1))
            back_msg[pl.ds(k, SUB, stride=depth), :] = value

        for a in range(lat_count):

            @pl.when(jnp.logical_or(lat != a, lat < 2))
            def _(a=a):
                back_copy(a).start()

        @pl.when(lat >= 2)
        def _():
            back_recv[odd] = back_msg[pl.ds(pl.multiple_of(lat * rows, rows), rows), :]

        for a in range(lat_count):

            @pl.when(jnp.logical_or(lat != a, lat < 2))
            def _(a=a):
                back_copy(a).wait_send()

    pl.when(is_owner)(solve_columns)

    for copy, stays in outgoing:
        if stays is None:
            copy.wait_send()
        else:
            pl.when(jnp.logical_not(stays))(copy.wait_send)

    for side in range(2):

        @pl.when(jnp.logical_or(core == 0, lat != 2 + side))
        def _(side=side):
            pltpu.make_async_remote_copy(
                src_ref=back_msg.at[0:rows],
                dst_ref=back_recv.at[side],
                send_sem=back_send.at[0],
                recv_sem=back_arrive.at[side],
                device_id=left_place,
                device_id_type=MESH,
            ).wait_recv()

    for v in range(rows // SUB):
        sl = slice(v * SUB, (v + 1) * SUB)
        first, second = back_recv[0, sl], back_recv[1, sl]
        sol_out[sl] = jnp.where(wide < own, first, second)
        res_out[sl] = pltpu.roll(jnp.where(wide < own, second, first), own, 1)


def shards(
    right_side,
    surface_term,
    east_coupling,
    north_coupling,
    neast_coupling,
    nwest_coupling,
    land_sea,
    fold_map,
):
    rows, width = right_side.shape
    lat_count = lax.axis_size("lat")
    lon_count = lax.axis_size("lon")
    n_own = lat_count * lon_count // 2
    depth = rows * lat_count // SUB
    subs = SUB // lat_count
    assert lat_count == 4 and ITERS % 2 == 0
    band = subs * (FIELDS // 2 * depth + depth // 2)
    thin = subs * depth // 2

    block = pltpu.VMEM((depth, SUB, width), jnp.float32)
    answer = jax.ShapeDtypeStruct((rows, width), jnp.float32)
    vmem = pl.BlockSpec(memory_space=pltpu.VMEM)
    dma = pltpu.SemaphoreType.DMA

    def held(*shape):
        return pltpu.VMEM((*shape, width), jnp.float32)

    return pl.pallas_call(
        functools.partial(kernel, lat_count, lon_count),
        out_shape=(answer, answer),
        in_specs=[pl.BlockSpec(memory_space=pl.ANY)] * 8,
        out_specs=(vmem, vmem),
        scratch_shapes=[block] * 25
        + [
            held(2, depth, SUB),
            held(2, depth, SUB),
            held(FIELDS, depth, SUB),
            held(FIELDS, rows),
            pltpu.VMEM((rows, width), jnp.int32),
            pltpu.SMEM((width,), jnp.int32),
            held(2, band),
            held(2, thin),
            held(lat_count * band),
            held(lat_count * thin),
            held(3, 1),
            held(n_own, 3, 1),
            held(7, lon_count),
            held(2, 2, 1),
            held(2, n_own, 2, 1),
            held(lat_count * rows),
            held(2, rows),
            dma((FIELDS + 2,)),
            dma((2,)),
            dma((lat_count,)),
            dma((2,)),
            dma((lat_count,)),
            dma(()),
            dma(()),
            dma((2,)),
            dma((2,)),
            dma((lat_count,)),
            dma((2,)),
        ],
        compiler_params=pltpu.CompilerParams(collective_id=0, has_side_effects=True),
    )(
        right_side,
        surface_term,
        east_coupling,
        north_coupling,
        neast_coupling,
        nwest_coupling,
        land_sea,
        fold_map,
    )


def solution(mesh):
    return jax.shard_map(
        shards,
        mesh=mesh,
        in_specs=(P("lat", "lon"),) * 7 + (P("lon"),),
        out_specs=(P("lat", "lon"), P("lat", "lon")),
        check_vma=False,
    )
```

```python
import functools

import jax
import jax.numpy as jnp
from jax import lax
from jax.experimental import pallas as pl
from jax.experimental.pallas import tpu as pltpu
from jax.sharding import PartitionSpec as P

ITERS = 8
SUB = 8
FIELDS = 6
MESH = pl.DeviceIdType.MESH


def iota(shape, dim):
    return lax.broadcasted_iota(jnp.int32, shape, dim)


def east(x):
    return pltpu.roll(x, x.shape[-1] - 1, x.ndim - 1)


def west(x):
    return pltpu.roll(x, 1, x.ndim - 1)


def from_above(x):
    return pltpu.roll(x, SUB - 1, 0)


def from_below(x):
    return pltpu.roll(x, 1, 0)


def alternate(size):
    ring = []
    for i in range(1, size // 2 + 1):
        ring += [size - i, i]
    return list(dict.fromkeys([*ring, 0]))


def kernel(
    lat_count,
    lon_count,
    right_ref,
    surface_ref,
    east_ref,
    north_ref,
    neast_ref,
    nwest_ref,
    land_ref,
    map_ref,
    sol_out,
    res_out,
    w_e,
    w_w,
    w_n,
    w_s,
    w_ne,
    w_sw,
    w_nw,
    w_se,
    diag,
    f_a,
    f_g,
    resp0,
    resp1,
    top_resp,
    c_mid,
    c_east,
    c_west,
    res_ref,
    basis,
    images,
    surf,
    o_mid,
    o_east,
    o_west,
    n_raw,
    g_east,
    g_west,
    given,
    land_buf,
    map_buf,
    big_msg,
    small_msg,
    big_recv,
    small_recv,
    stat_msg,
    stat_recv,
    msg,
    recv,
    back_msg,
    back_recv,
    in_sem,
    big_send,
    big_arrive,
    small_send,
    small_arrive,
    stat_send,
    stat_arrive,
    send_sem,
    recv_sem,
    back_send,
    back_arrive,
):
    pairs = lon_count // 2
    n_own = lat_count * pairs
    lat = lax.axis_index("lat")
    lon = lax.axis_index("lon")
    pair = lon // 2
    core = lax.rem(lon, 2)
    me = lat * pairs + pair
    depth, _, width = res_ref.shape
    rows = depth * SUB // lat_count
    subs = SUB // lat_count
    halo = ITERS
    own = 2 * width // lat_count
    big = own + halo
    rest = width - big
    band = big_msg.shape[2]
    thin = small_msg.shape[2]
    seg = band // subs
    half = depth // 2
    top = depth - 1
    odd = lax.rem(lat, 2)
    is_owner = core == 1

    lats = [lax.rem(lat + d, lat_count) for d in range(lat_count)]
    owners = [2 * lax.rem(pair + d, pairs) + 1 for d in range(pairs)]
    few = n_own <= 64
    peers = [(p, q) for q in alternate(pairs) for p in alternate(lat_count) if p or q]

    def to_owners(act):
        if few:
            for p, q in peers:
                act((lats[p], owners[q]))
            return

        def one(step, carry):
            peer = lax.rem(me + step, n_own)
            act((peer // pairs, 2 * lax.rem(peer, pairs) + 1))
            return carry

        lax.fori_loop(1, n_own, one, 0)

    left_place = (2 * core, 2 * pair + 1)
    right_place = (2 * core + 1, 2 * pair + 1)
    next_place = (lax.rem(2 * core + 2, lat_count), 2 * lax.rem(pair + core, pairs) + 1)
    back_pair = lax.rem(pair + core + pairs - 1, pairs)
    prev_place = (lax.rem(2 * core + 3, lat_count), 2 * back_pair + 1)

    barrier = pltpu.get_barrier_semaphore()

    def greet(place):
        pl.semaphore_signal(barrier, inc=1, device_id=place, device_id_type=MESH)

    @pl.when(is_owner)
    def _():
        to_owners(greet)
        last_lat = jnp.where(lat == lat_count - 1, 1, 0)
        plain = 2 * lax.rem(pair + last_lat, pairs)
        for a in range(lat_count):
            greet((a, plain))

    @pl.when(core == 0)
    def _():
        for place in (left_place, right_place, next_place, prev_place):
            greet(place)

    sources = (surface_ref, north_ref, right_ref, east_ref, neast_ref, nwest_ref)
    loads = [
        pltpu.make_async_copy(ref, given.at[i], in_sem.at[i]) for i, ref in enumerate(sources)
    ]
    land_load = pltpu.make_async_copy(land_ref, land_buf, in_sem.at[FIELDS])
    map_load = pltpu.make_async_copy(map_ref, map_buf, in_sem.at[FIELDS + 1])
    land_load.start()
    for copy in loads:
        copy.start()
    map_load.start()

    wide = iota((SUB, width), 1)
    zero = jnp.zeros((SUB, width), jnp.float32)
    sixteenth = wide // halo
    groups = width // halo
    here_big = pl.ds(pl.multiple_of(lat * band, SUB), band)
    here_thin = pl.ds(pl.multiple_of(lat * thin, SUB), thin)

    def big_copy(side, c):
        return pltpu.make_async_remote_copy(
            src_ref=big_msg.at[side, c],
            dst_ref=big_recv.at[c, here_big],
            send_sem=big_send.at[side, c],
            recv_sem=big_arrive.at[c, lat],
            device_id=(left_place, right_place)[side],
            device_id_type=MESH,
        )

    def thin_copy(side, c):
        return pltpu.make_async_remote_copy(
            src_ref=small_msg.at[side, c],
            dst_ref=small_recv.at[c, here_thin],
            send_sem=small_send.at[side, c],
            recv_sem=small_arrive.at[c, lat],
            device_id=(next_place, prev_place)[side],
            device_id_type=MESH,
        )

    big_stays = [jnp.logical_and(is_owner, lat == 2 + side) for side in range(2)]
    thin_stays = jnp.logical_and(is_owner, lat == 1)

    def pack(c):
        for s in range(subs):
            for v in range(depth // SUB):
                sl = slice(s * depth + v * SUB, s * depth + (v + 1) * SUB)
                first, second = given[2 * c, sl], given[2 * c + 1, sl]
                second = pltpu.roll(second, own, 1)
                at = s * seg + v * SUB
                to = slice(at, at + SUB)
                big_msg[0, c, to] = jnp.where(wide < big, first, second)
                big_msg[1, c, to] = jnp.where(wide >= rest, first, second)
            acc_l, acc_r, acc_n, acc_p = zero, zero, zero, zero
            for j in range(SUB):
                phase = pl.ds(s * depth + j, SUB, stride=SUB)
                first, second = given[2 * c, phase, :], given[2 * c + 1, phase, :]
                lane = halo * j
                even_b = pltpu.roll(second, (lane + own) % width, 1)
                odd_b = pltpu.roll(second, lane + halo, 1)
                even_a = pltpu.roll(first, lane, 1) if lane else first
                odd_a = pltpu.roll(first, (lane + own + halo) % width, 1)
                hit = lax.rem(sixteenth, groups // 2) == j
                acc_l = jnp.where(hit, even_b, acc_l)
                acc_r = jnp.where(hit, odd_b, acc_r)
                acc_n = jnp.where(sixteenth == (j + groups - 1) % groups, even_a, acc_n)
                acc_n = jnp.where(sixteenth == (j + groups // 2 - 1) % groups, even_b, acc_n)
                acc_p = jnp.where(sixteenth == (j + groups // 2 + 1) % groups, odd_a, acc_p)
                acc_p = jnp.where(sixteenth == (j + 1) % groups, odd_b, acc_p)
            at = s * seg + depth
            big_msg[0, c, at : at + SUB] = acc_l
            big_msg[1, c, at : at + SUB] = acc_r
            at = s * SUB
            small_msg[0, c, at : at + SUB] = acc_n
            small_msg[1, c, at : at + SUB] = acc_p

    def send(c):
        for side in range(2):
            pl.when(jnp.logical_not(big_stays[side]))(big_copy(side, c).start)

            @pl.when(big_stays[side])
            def _(side=side):
                pltpu.make_async_copy(
                    big_msg.at[side, c], big_recv.at[c, here_big], big_arrive.at[c, lat]
                ).start()

        thin_copy(0, c).start()
        pl.when(jnp.logical_not(thin_stays))(thin_copy(1, c).start)

        @pl.when(thin_stays)
        def _():
            pltpu.make_async_copy(
                small_msg.at[1, c], small_recv.at[c, here_thin], small_arrive.at[c, lat]
            ).start()

    land_load.wait()
    for c in range(FIELDS // 2):
        loads[2 * c].wait()
        loads[2 * c + 1].wait()
        if c == 0:
            for v in range(rows // SUB):
                sl = slice(v * SUB, (v + 1) * SUB)
                given[0, sl] = given[0, sl] * land_buf[sl].astype(jnp.float32)
        pack(c)
        if c == 0:

            @pl.when(is_owner)
            def _():
                pl.semaphore_wait(barrier, n_own - 1 + lat_count)

            @pl.when(core == 0)
            def _():
                pl.semaphore_wait(barrier, lat_count)

        send(c)
    map_load.wait()

    def back_copy(a):
        return pltpu.make_async_remote_copy(
            src_ref=back_msg.at[a * rows : (a + 1) * rows],
            dst_ref=back_recv.at[odd],
            send_sem=back_send.at[a],
            recv_sem=back_arrive.at[odd],
            device_id=(a, 2 * pair + lat // 2),
            device_id_type=MESH,
        )

    def solve_columns():
        def receive(c):
            for a in range(lat_count):
                pltpu.make_async_remote_copy(
                    src_ref=big_msg.at[0, c],
                    dst_ref=big_recv.at[c, a * band : (a + 1) * band],
                    send_sem=big_send.at[0, c],
                    recv_sem=big_arrive.at[c, a],
                    device_id=left_place,
                    device_id_type=MESH,
                ).wait_recv()
                pltpu.make_async_remote_copy(
                    src_ref=small_msg.at[0, c],
                    dst_ref=small_recv.at[c, a * thin : (a + 1) * thin],
                    send_sem=small_send.at[0, c],
                    recv_sem=small_arrive.at[c, a],
                    device_id=next_place,
                    device_id_type=MESH,
                ).wait_recv()

        def between(low, size):
            return (wide >= low) & (wide < low + size)

        native = between(odd * rest, big)
        side = between((1 - odd) * (width - halo), halo)
        ends = between(own - halo, 2 * halo) | between(odd * (width - halo), halo)
        strip_hit = [
            lax.rem(sixteenth, groups // 2) == lax.rem(j + groups // 2 - 1 + 2 * odd, groups // 2)
            for j in range(SUB)
        ]
        shifts = [lax.rem(odd * rest - halo * j + width, width) for j in range(SUB)]

        def unpack(c, k):
            j = k % SUB
            strip = small_recv[c, pl.ds(k // SUB, SUB, stride=SUB), :]
            spill = big_recv[c, pl.ds(depth + k // SUB, SUB, stride=seg), :]
            packed = big_recv[c, pl.ds(k, SUB, stride=seg), :]
            moved = pltpu.roll(jnp.where(strip_hit[j], strip, spill), shifts[j], 1)
            first = jnp.where(native, packed, jnp.where(side, moved, 0.0))
            second = jnp.where(native, jnp.where(ends, moved, 0.0), packed)
            return first, pltpu.roll(second, own, 1)

        is_top = iota((SUB, width), 0) == SUB - 1

        def shut(value, k):
            return jnp.where(is_top, 0.0, value) if k == top else value

        def is_ocean(surface):
            return jnp.where(surface > 0.0, 1.0, 0.0)

        receive(0)
        below_north = None
        for k in range(depth):
            surface, north = unpack(0, k)
            ocean = is_ocean(surface)
            surf[k] = surface
            o_mid[k] = ocean
            o_east[k] = east(ocean)
            o_west[k] = west(ocean)
            n_raw[k] = north
            if k:
                wn = below_north * ocean
                w_n[k - 1] = wn
                w_s[k] = wn
            below_north = shut(north, k) * ocean
        wn = below_north * from_above(o_mid[0])
        w_n[top] = wn
        w_s[0] = from_below(wn)

        def line_surface(k):
            return surf[k] + (1.0 - o_mid[k])

        low = line_surface(0) + w_s[0]
        high = line_surface(top) + w_n[top]
        for k in range(half):
            up, j = k, top - k
            g_low = 1.0 / (low + w_n[up])
            g_high = 1.0 / (high + w_s[j])
            f_g[up] = g_low
            f_g[j] = g_high
            if k < half - 1:
                f_a[up + 1] = w_n[up] * g_low
                f_a[j - 1] = w_s[j] * g_high
                low = line_surface(up + 1) + w_n[up] * (low * g_low)
                high = line_surface(j - 1) + w_s[j] * (high * g_high)
        mid = w_n[half - 1]
        inv_det = 1.0 / (low * high + mid * (low + high))
        mid_ll = (high + mid) * inv_det
        mid_lh = mid * inv_det
        mid_hh = (low + mid) * inv_det

        def line(read, out, u_ref):
            y, z = read(0), read(top)
            u_ref[0] = y
            u_ref[top] = z
            for k in range(1, half):
                j = top - k
                y = read(k) + f_a[k] * y
                z = read(j) + f_a[j] * z
                u_ref[k] = y
                u_ref[j] = z
            x = mid_ll * y + mid_lh * z
            v = mid_lh * y + mid_hh * z
            out[half - 1] = x
            out[half] = v
            for k in range(half - 2, -1, -1):
                j = top - k
                x = f_g[k] * u_ref[k] + f_a[k + 1] * x
                v = f_g[j] * u_ref[j] + f_a[j - 1] * v
                out[k] = x
                out[j] = v

        line(lambda k: w_s[0] if k == 0 else zero, resp0, images.at[0])
        line(lambda k: w_n[top] if k == top else zero, resp1, images.at[0])

        a, b, c, d = resp0[0], resp1[0], resp0[top], resp1[top]
        plan = []
        stride = 1
        while stride < SUB:
            cb, db = pltpu.roll(c, stride, 0), pltpu.roll(d, stride, 0)
            aa, ba = pltpu.roll(a, SUB - stride, 0), pltpu.roll(b, SUB - stride, 0)
            m00, m01 = 1.0 - a * db, -b * aa
            m10, m11 = -c * db, 1.0 - d * aa
            inv = 1.0 / (m00 * m11 - m01 * m10)
            i00, i01, i10, i11 = m11 * inv, -m01 * inv, -m10 * inv, m00 * inv
            t0, t1 = i00 * a + i01 * c, i00 * b + i01 * d
            t2, t3 = i10 * a + i11 * c, i10 * b + i11 * d
            plan.append((stride, i00, i01, i10, i11, t0, t1, t2, t3))
            a, b, c, d = t0 * cb, t1 * ba, t2 * cb, t3 * ba
            stride *= 2

        def interface(p, q):
            for stride, i00, i01, i10, i11, t0, t1, t2, t3 in plan:
                qb = pltpu.roll(q, stride, 0)
                pa = pltpu.roll(p, SUB - stride, 0)
                p, q = (
                    (i00 * p + i01 * q) + (t0 * qb + t1 * pa),
                    (i10 * p + i11 * q) + (t2 * qb + t3 * pa),
                )
            return from_below(q), from_above(p)

        def solve(read, u_ref):
            line(read, u_ref, u_ref)
            below, over = interface(u_ref[0], u_ref[top])

            def finish(k):
                value = u_ref[k] + below * resp0[k] + over * resp1[k]
                u_ref[k] = value
                return value

            return finish

        def walk(finish):
            last = finish(top)
            first = finish(0)
            last = (last, east(last), west(last))
            first = (first, east(first), west(first))
            prev = tuple(from_below(x) for x in last)
            now = first
            for k in range(depth):
                if k < top - 1:
                    value = finish(k + 1)
                    nxt = (value, east(value), west(value))
                elif k == top - 1:
                    nxt = last
                else:
                    nxt = tuple(from_above(x) for x in first)
                yield k, prev, now, nxt
                prev, now = now, nxt

        def column_sum(x):
            return jnp.sum(x, axis=0, keepdims=True)

        lane = iota((1, width), 1)
        relative = lax.rem(lane - odd * own + width, width)
        own_row = relative < own

        unit = jnp.where(is_top, 1.0, 0.0)
        finish = solve(lambda k: unit if k == top else zero, top_resp)
        for k in range(depth):
            value = finish(k)
            g_east[k] = east(value)
            g_west[k] = west(value)

        receive(1)
        n_prev = from_below(shut(n_raw[top], top))
        for k in range(depth):
            right, eastern = unpack(1, k)
            ocean = o_mid[k]
            inner = west(eastern)
            w_e[k] = eastern * ocean * o_east[k]
            w_w[k] = inner * ocean * o_west[k]
            n_now = shut(n_raw[k], k)
            diag[k] = eastern + inner + n_now + n_prev
            n_prev = n_now
            res_ref[k] = ocean * right

        receive(2)

        def corners(k):
            ne, nw = (shut(x, k) for x in unpack(2, k))
            ne_west, nw_east = west(ne), east(nw)
            if k < top:
                next_mid, next_east, next_west = o_mid[k + 1], o_east[k + 1], o_west[k + 1]
            else:
                next_mid, next_east, next_west = (
                    from_above(x[0]) for x in (o_mid, o_east, o_west)
                )
            ocean = o_mid[k]
            wne, wnw = ne * ocean * next_east, nw * ocean * next_west
            sw, se = ne_west * o_west[k] * next_mid, nw_east * o_east[k] * next_mid
            w_ne[k] = wne
            w_nw[k] = wnw
            return ne + nw, ne_west + nw_east, sw, se, wne, wnw

        last = corners(top)
        sum_prev, sw, se = (from_below(x) for x in (last[1], last[2], last[3]))
        h_mid, h_east = zero, zero
        for k in range(depth):
            now = corners(k) if k < top else last
            ocean = o_mid[k]
            value = surf[k] + ocean * (diag[k] + now[0] + sum_prev) + (1.0 - ocean)
            diag[k] = value
            w_sw[k] = sw
            w_se[k] = se
            around = (top_resp, g_east, g_west)
            prev = [x[k - 1] if k else from_below(x[top]) for x in around]
            nxt = [x[k + 1] if k < top else from_above(x[0]) for x in around]
            here = top_resp[k]
            middle = value * here - w_n[k] * nxt[0] - w_s[k] * prev[0]
            eastern = -(w_e[k] * g_east[k] + now[4] * nxt[1] + se * prev[1])
            c_mid[k] = middle
            c_east[k] = eastern
            c_west[k] = -(w_w[k] * g_west[k] + now[5] * nxt[2] + sw * prev[2])
            h_mid = h_mid + here * middle
            h_east = h_east + here * eastern
            sum_prev, sw, se = now[1], now[2], now[3]

        def both(native_row, other_row):
            return jnp.where(own_row, native_row, pltpu.roll(other_row, own, 1))

        def last_row(x):
            return x[SUB - 1 :]

        stat_msg[0] = both(last_row(top_resp[top]), column_sum(h_mid))
        stat_msg[1] = both(column_sum(h_east), last_row(n_raw[top]))
        stat_msg[2] = both(last_row(o_mid[top]), jnp.zeros((1, width), jnp.float32))
        stat_recv[me] = stat_msg[...]

        def stat_start(place):
            pltpu.make_async_remote_copy(
                src_ref=stat_msg,
                dst_ref=stat_recv.at[me],
                send_sem=stat_send,
                recv_sem=stat_arrive,
                device_id=place,
                device_id_type=MESH,
            ).start()

        to_owners(stat_start)

        def send_rows(b):
            def start(place):
                pltpu.make_async_remote_copy(
                    src_ref=msg.at[b],
                    dst_ref=recv.at[b, me],
                    send_sem=send_sem.at[b],
                    recv_sem=recv_sem.at[b],
                    device_id=place,
                    device_id_type=MESH,
                ).start()

            to_owners(start)

        def wait_for(every, sent, arrived):
            pltpu.make_async_remote_copy(
                src_ref=every,
                dst_ref=every,
                send_sem=sent,
                recv_sem=arrived,
                device_id=next_place,
                device_id_type=MESH,
            ).wait()

        lanes = iota((lon_count, width), 1)
        rows_id = iota((lon_count, width), 0)

        def assemble(read):
            lefts, rights = [], []
            for block in range(lon_count):
                spot = 2 * (block % 2) * pairs + block // 2
                lefts.append(read(spot))
                rights.append(read(spot + pairs))
            lefts = jnp.concatenate(lefts, axis=0)
            rights = jnp.concatenate(rights, axis=0)
            native_rows = jnp.where(lanes < own, lefts, rights)
            other_rows = pltpu.roll(jnp.where(lanes < own, rights, lefts), own, 1)
            return native_rows, other_rows

        total_cols = lon_count * width
        turn = lax.rem(map_buf[0] + lon * width, total_cols)
        back = total_cols - 1 - turn
        row_shift = back // width
        lane_shift = lax.rem(back, width)
        turn_index = width - 1 - lax.rem(lanes + lane_shift, width)

        def facing(x):
            flipped = jnp.concatenate(
                [x[b : b + 1] for b in range(lon_count - 1, -1, -1)], axis=0
            )
            moved = jnp.take_along_axis(flipped, turn_index, axis=1)
            first = pltpu.roll(moved, lax.rem(lon_count - row_shift, lon_count), 0)
            second = pltpu.roll(moved, lon_count - 1 - row_shift, 0)
            return jnp.where(lanes + lane_shift < width, first, second)

        block_row = 2 * pair + lat // 2
        odd_home = jnp.where(lanes < own // 2, 1, 0)
        even_home = jnp.where(lanes >= width - own // 2, -1, 0)
        home = block_row + odd * odd_home + (1 - odd) * even_home
        pick = rows_id == lax.rem(home + lon_count, lon_count)

        def window(x):
            return jnp.sum(jnp.where(pick, x, 0.0), axis=0, keepdims=True)

        def spread(x):
            return jnp.broadcast_to(x, (SUB, width))

        def total(x):
            return jnp.sum(x, keepdims=True)

        def east_whole(x):
            moved = east(x)
            return jnp.where(lanes == width - 1, pltpu.roll(moved, lon_count - 1, 0), moved)

        def west_whole(x):
            moved = west(x)
            return jnp.where(lanes == 0, pltpu.roll(moved, 1, 0), moved)

        def stencil(k, prev, now, nxt):
            return (
                (diag[k] * now[0] - w_e[k] * now[1] - w_w[k] * now[2])
                - (w_n[k] * nxt[0] + w_ne[k] * nxt[1] + w_nw[k] * nxt[2])
                - (w_s[k] * prev[0] + w_se[k] * prev[1] + w_sw[k] * prev[2])
            )

        def product(p, q):
            return [[p[i][0] * q[0][j] + p[i][1] * q[1][j] for j in (0, 1)] for i in (0, 1)]

        def turned_product(p, q):
            return [[p[0][i] * q[0][j] + p[1][i] * q[1][j] for j in (0, 1)] for i in (0, 1)]

        def plus(p, q):
            return [[p[i][j] + q[i][j] for j in (0, 1)] for i in (0, 1)]

        def minus(p, q):
            return [[p[i][j] - q[i][j] for j in (0, 1)] for i in (0, 1)]

        def factor(p):
            first = 1.0 / p[0][0]
            slope = p[0][1] * first
            return first, slope, 1.0 / (p[1][1] - slope * p[0][1]), p[0][1]

        def solve_pair(f, u, v):
            second = (v - f[1] * u) * f[2]
            return (u - f[3] * second) * f[0], second

        blocks = ITERS // 2
        factors, links, tails, phi_rows = [], {}, [], []
        weight_of = [[0.0, 0.0] for _ in range(blocks)]
        rest_lane = lax.rem(lane, own)
        for b in range(blocks):
            z_ref, k_ref = basis.at[2 * b], basis.at[2 * b + 1]
            y_ref, w_ref = images.at[2 * b], images.at[2 * b + 1]
            acc = [zero] * 9
            old = [zero] * (4 * b)
            for k, prev, now, nxt in walk(solve(lambda k: res_ref[k], z_ref)):
                value = stencil(k, prev, now, nxt)
                y_ref[k] = value
                acc[k % 2] = acc[k % 2] + res_ref[k] * now[0]
                acc[2 + k % 2] = acc[2 + k % 2] + now[0] * value
                for j in range(b):
                    old[4 * j] = old[4 * j] + now[0] * images[2 * j, k]
                    old[4 * j + 1] = old[4 * j + 1] + now[0] * images[2 * j + 1, k]
                    old[4 * j + 3] = old[4 * j + 3] + res_ref[k] * basis[2 * j, k]
            for k, prev, now, nxt in walk(solve(lambda k: y_ref[k], k_ref)):
                value = stencil(k, prev, now, nxt)
                w_ref[k] = value
                acc[4 + k % 2] = acc[4 + k % 2] + y_ref[k] * now[0]
                acc[6 + k % 2] = acc[6 + k % 2] + now[0] * value
                acc[8] = acc[8] + top_resp[k] * value
                for j in range(b):
                    old[4 * j + 2] = old[4 * j + 2] + now[0] * images[2 * j + 1, k]
            fields = [acc[2 * i] + acc[2 * i + 1] for i in range(4)] + old
            sums = jnp.zeros((1, width), jnp.float32)
            for i, x in enumerate(fields):
                sums = jnp.where(relative == own + i, total(jnp.where(own_row, x, 0.0)), sums)
            msg[b, 0] = both(last_row(z_ref[top]), last_row(k_ref[top]))
            msg[b, 1] = jnp.where(own_row, column_sum(acc[8]), sums)
            recv[b, me] = msg[b]
            send_rows(b)

            if b == 0:
                wait_for(stat_recv.at[0 : n_own - 1], stat_send, stat_arrive)
                h0, h1 = assemble(lambda spot: stat_recv[spot, 0])
                h2, north = assemble(lambda spot: stat_recv[spot, 1])
                ocean, _ = assemble(lambda spot: stat_recv[spot, 2])
                fold_open = 0.5 * (north + facing(north))
                fold_own = fold_open * ocean
                fold_far = fold_own * facing(ocean)
                h0_facing, own_facing = facing(h0), facing(fold_own)

            wait_for(recv.at[b, 0 : n_own - 1], send_sem.at[b], recv_sem.at[b])
            tau0, tau1 = assemble(lambda spot, b=b: recv[b, spot, 0])
            tail, rest_rows = assemble(lambda spot, b=b: recv[b, spot, 1])
            tau0_facing, tau1_facing = facing(tau0), facing(tau1)
            phi0 = fold_far * tau0_facing - fold_own * tau0
            phi0_facing = fold_far * tau0 - own_facing * tau0_facing
            top1 = tau1 - h0 * phi0
            phi1 = fold_far * (tau1_facing - h0_facing * phi0_facing) - fold_own * top1
            spread_phi = h1 * phi0 + h2 * east_whole(phi0) + west_whole(h2 * phi0)
            rest_sum = column_sum(rest_rows)

            def moment(i, x=None):
                row = jnp.where(rest_lane == i, rest_sum, 0.0)
                if x is not None:
                    row = row + column_sum(x)
                return jnp.sum(row, axis=1, keepdims=True)

            m0 = moment(0)
            m1 = moment(1, -tau0 * phi0)
            m2 = moment(2, phi0 * (h0 * phi0 - 2.0 * tau1))
            m3 = moment(3, phi0 * (spread_phi - 2.0 * tail) - top1 * phi1)
            cross, ends_of = [], []
            for j in range(b):
                first, mixed = moment(4 + 4 * j), moment(5 + 4 * j)
                last = moment(6 + 4 * j, -phi0 * tails[j])
                cross.append([[first, mixed], [mixed, last]])
                ends_of.append([moment(7 + 4 * j), first])
            ends_of.append([m0, m1])
            tails.append(tail - spread_phi - h0 * phi1)
            phi0_row, phi1_row = window(phi0), window(phi1)
            phi_rows.append(phi0_row)

            inner = [[m1, m2], [m2, m3]]
            pulls = []
            for j in range(b):
                against = cross[j]
                for i in range(j):
                    against = plus(against, turned_product(links[i, j], cross[i]))
                left = solve_pair(factors[j], against[0][0], against[1][0])
                right = solve_pair(factors[j], against[0][1], against[1][1])
                pulls.append([[left[0], right[0]], [left[1], right[1]]])
                inner = minus(inner, turned_product(against, pulls[j]))
            factors.append(factor(inner))
            for j in range(b):
                link = [[-x for x in row] for row in pulls[j]]
                for i in range(j + 1, b):
                    link = minus(link, product(links[j, i], pulls[i]))
                links[j, b] = link
            along = []
            for j in range(b + 1):
                u, v = ends_of[j]
                for i in range(j):
                    link, (p, q) = links[i, j], ends_of[i]
                    u = u + (link[0][0] * p + link[1][0] * q)
                    v = v + (link[0][1] * p + link[1][1] * q)
                along.append(solve_pair(factors[j], u, v))
            steps = []
            for j in range(b + 1):
                u, v = along[j]
                for i in range(j + 1, b + 1):
                    link, (p, q) = links[j, i], along[i]
                    u = u + (link[0][0] * p + link[0][1] * q)
                    v = v + (link[1][0] * p + link[1][1] * q)
                steps.append([u, v])
            for j in range(b + 1):
                weight_of[j] = [weight_of[j][i] + steps[j][i] for i in (0, 1)]
            wide_steps = [[spread(x) for x in row] for row in steps]
            p_mid, p_east, p_west = (
                spread(phi0_row),
                spread(east(phi0_row)),
                spread(west(phi0_row)),
            )
            phi1_top = jnp.where(is_top, spread(phi1_row), 0.0)
            phi0_top = jnp.where(is_top, p_mid, 0.0)
            final = b == blocks - 1
            if final:
                wide_weights = [[spread(x) for x in row] for row in weight_of]
                phi_sum = zero
                for j in range(blocks):
                    phi_sum = phi_sum + wide_weights[j][1] * phi_rows[j]
            for k in range(depth):
                image = y_ref[k]
                second = w_ref[k] - (c_mid[k] * p_mid + c_east[k] * p_east + c_west[k] * p_west)
                if k == top:
                    image = image - phi0_top
                    second = second - phi1_top
                value = res_ref[k] - (wide_steps[b][0] * image + wide_steps[b][1] * second)
                for j in range(b):
                    value = value - (
                        wide_steps[j][0] * images[2 * j, k]
                        + wide_steps[j][1] * images[2 * j + 1, k]
                    )
                if not final:
                    if k == top:
                        y_ref[k] = image
                    w_ref[k] = second
                    res_ref[k] = value
                    continue
                answer = -top_resp[k] * phi_sum
                for j in range(blocks):
                    answer = answer + (
                        wide_weights[j][0] * basis[2 * j, k]
                        + wide_weights[j][1] * basis[2 * j + 1, k]
                    )
                joined = jnp.where(own_row, answer, pltpu.roll(value, own, 1))
                back_msg[pl.ds(k, SUB, stride=depth), :] = joined

        for a in range(lat_count):

            @pl.when(jnp.logical_or(lat != a, lat < 2))
            def _(a=a):
                back_copy(a).start()

        @pl.when(lat >= 2)
        def _():
            back_recv[odd] = back_msg[pl.ds(pl.multiple_of(lat * rows, rows), rows), :]

        for a in range(lat_count):

            @pl.when(jnp.logical_or(lat != a, lat < 2))
            def _(a=a):
                back_copy(a).wait_send()

    pl.when(is_owner)(solve_columns)

    for c in range(FIELDS // 2):
        for side in range(2):
            pl.when(jnp.logical_not(big_stays[side]))(big_copy(side, c).wait_send)
        thin_copy(0, c).wait_send()
        pl.when(jnp.logical_not(thin_stays))(thin_copy(1, c).wait_send)

    for side in range(2):

        @pl.when(jnp.logical_or(core == 0, lat != 2 + side))
        def _(side=side):
            pltpu.make_async_remote_copy(
                src_ref=back_msg.at[0:rows],
                dst_ref=back_recv.at[side],
                send_sem=back_send.at[0],
                recv_sem=back_arrive.at[side],
                device_id=left_place,
                device_id_type=MESH,
            ).wait_recv()

    for v in range(rows // SUB):
        sl = slice(v * SUB, (v + 1) * SUB)
        first, second = back_recv[0, sl], back_recv[1, sl]
        sol_out[sl] = jnp.where(wide < own, first, second)
        res_out[sl] = pltpu.roll(jnp.where(wide < own, second, first), own, 1)


def shards(
    right_side,
    surface_term,
    east_coupling,
    north_coupling,
    neast_coupling,
    nwest_coupling,
    land_sea,
    fold_map,
):
    rows, width = right_side.shape
    lat_count = lax.axis_size("lat")
    lon_count = lax.axis_size("lon")
    n_own = lat_count * lon_count // 2
    depth = rows * lat_count // SUB
    subs = SUB // lat_count
    assert lat_count == 4 and ITERS % 2 == 0
    band = subs * (depth + SUB)
    thin = subs * SUB

    block = pltpu.VMEM((depth, SUB, width), jnp.float32)
    answer = pltpu.VMEM((rows, width), jnp.float32)
    vmem = pl.BlockSpec(memory_space=pltpu.VMEM)
    dma = pltpu.SemaphoreType.DMA

    def held(*shape):
        return pltpu.VMEM((*shape, width), jnp.float32)

    return pl.pallas_call(
        functools.partial(kernel, lat_count, lon_count),
        out_shape=(answer, answer),
        in_specs=[pl.BlockSpec(memory_space=pl.ANY)] * 8,
        out_specs=(vmem, vmem),
        scratch_shapes=[block] * 18
        + [
            held(ITERS, depth, SUB),
            held(ITERS, depth, SUB),
            *[held(depth, SUB)] * 7,
            held(FIELDS, rows),
            pltpu.VMEM((rows, width), jnp.int32),
            pltpu.SMEM((width,), jnp.int32),
            held(2, FIELDS // 2, band),
            held(2, FIELDS // 2, thin),
            held(FIELDS // 2, lat_count * band),
            held(FIELDS // 2, lat_count * thin),
            held(3, 1),
            held(n_own, 3, 1),
            held(ITERS // 2, 2, 1),
            held(ITERS // 2, n_own, 2, 1),
            held(lat_count * rows),
            held(2, rows),
            dma((FIELDS + 2,)),
            dma((2, FIELDS // 2)),
            dma((FIELDS // 2, lat_count)),
            dma((2, FIELDS // 2)),
            dma((FIELDS // 2, lat_count)),
            dma(()),
            dma(()),
            dma((ITERS // 2,)),
            dma((ITERS // 2,)),
            dma((lat_count,)),
            dma((2,)),
        ],
        compiler_params=pltpu.CompilerParams(collective_id=0, has_side_effects=True),
    )(
        right_side,
        surface_term,
        east_coupling,
        north_coupling,
        neast_coupling,
        nwest_coupling,
        land_sea,
        fold_map,
    )


def solution(mesh):
    return jax.shard_map(
        shards,
        mesh=mesh,
        in_specs=(P("lat", "lon"),) * 7 + (P("lon"),),
        out_specs=(P("lat", "lon"), P("lat", "lon")),
        check_vma=False,
    )
```
